32 devices in a mesh: sims: 2 (over x), rows: 4 (over y, core), fields: 4 (over z).
Axes of the slice: x: 2, y: 2, z: 4, core: 2. Of those that a mesh axis runs over, the one named last changes fastest.
Arguments:
- sky_maps: float32 [6, 32, 16384], P('sims', 'rows', 'fields'), parts along dimension 0, may hold values from -7 to 7
- band_cuts: int32 [6], replicated, may hold values from 1 to 8191, as said below
- filters: float32 [3, 32, 16384], P(None, ('rows', 'fields')), may hold values from 0.3 to 3
- wiener: float32 [2, 32, 16384], P(None, ('rows', 'fields')), may hold values from 0.3 to 3
- response: float32 [32, 16384], P(('rows', 'fields')), may hold values from 0.5 to 2
Outputs:
- phi_curl: float32 [4, 32, 16384], P('sims', 'rows', 'fields'), parts along dimension 0
The draws below stay inside these ranges and needn't reach their ends.
There are 2 independent parts, one for each index of `sims`. The reference program is written for one: setup_inputs(seed, part) draws one part's arguments, and reference() takes and returns one part's arrays. A program takes and returns all parts, laid end to end along the dimension named above; an argument that names none is the same for every part. Nothing has to cross between parts.
Inputs may be any that keep to these rules, and one draw needn't show every extreme that they name: `band_cuts`: entries 0, 2 and 4 are the smallest multipole indices of the temperature, polarization and estimate bands and lie below 512; entries 1, 3 and 5 are the largest and are at least 4096.
All inputs are finite; a program needn't handle non-finite values.
Results may differ from the reference program's by a relative error of at most 0.00019.
Values sent between devices are 32-bit elements; how exact they have to be, the bound alone decides.
No kernel may reach another device: no remote copies, remote signals or barrier semaphores. Data moves between devices by JAX's collectives and lax.ppermute only.
A program may use at most 128 MiB of HBM per device.

```python
import math
import jax
import jax.numpy as jnp

NC = 16384
NR = 32


def draw_sky_maps(key, part):
    rough_part = jax.random.normal(key, (3, NR, NC), jnp.float32)
    return jnp.clip(rough_part, -7.0, 7.0)


def draw_band_cuts(key, part):
    low_key = jax.random.fold_in(key, 3)
    high_key = jax.random.fold_in(key, 5)
    lowest = jax.random.randint(low_key, (3,), 1, max(2, NC // 32), dtype=jnp.int32)
    highest = jax.random.randint(high_key, (3,), NC // 4, NC // 2, dtype=jnp.int32)
    return jnp.stack([lowest, highest], axis=1).reshape(6)


def steps_of(own_key, shape, split, smallest, top_value):
    factor_of, own = 1.0, jax.random.fold_in(own_key, 6)
    for dim, parts in split:
        heights = jnp.exp(jax.random.uniform(jax.random.fold_in(own, dim), (parts,), jnp.float32, smallest / len(split), top_value / len(split)))
        factor_of = factor_of * jnp.repeat(heights, shape[dim] // parts).reshape([-1 if axis == dim else 1 for axis in range(len(shape))])
    return factor_of


def setup_inputs(seed: int = 0, part: int = 0) -> dict:
    keys = jax.random.split(jax.random.key(seed), 6)
    own_keys = jax.random.split(jax.random.fold_in(keys[5], part), 6)
    return {
        "sky_maps": draw_sky_maps(jax.random.fold_in(jax.random.fold_in(keys[5], part), 71), part),
        "band_cuts": draw_band_cuts(jax.random.fold_in(keys[5], 71), part),
        "filters": jnp.clip(jnp.exp(math.log(3.0) - 2.3025851 * jax.random.uniform(keys[2], (3, NR, NC), jnp.float32) ** steps_of(keys[2], (3, NR, NC), ((1, 16),), -0.2, 0.2)), 0.3, 3.0),
        "wiener": jnp.clip(jnp.exp(math.log(3.0) - 2.3025851 * jax.random.uniform(keys[3], (2, NR, NC), jnp.float32) ** steps_of(keys[3], (2, NR, NC), ((1, 16),), -0.2, 0.2)), 0.3, 3.0),
        "response": jnp.clip(jnp.exp(math.log(2.0) - 1.3862944 * jax.random.uniform(keys[4], (NR, NC), jnp.float32) ** steps_of(keys[4], (NR, NC), ((0, 16),), -0.2, 0.2)), 0.5, 2.0),
    }


def signed_index(length):
    indices = jnp.arange(length, dtype=jnp.int32)
    return jnp.where(indices < length // 2, indices, indices - length)


def reference(sky_maps, band_cuts, filters, wiener, response):
    row_ratio = NC // NR
    freq_rows = signed_index(NR)[:, None]
    freq_cols = signed_index(NC)[None, :]
    scaled_rows = row_ratio * freq_rows
    radius_sq = freq_cols * freq_cols + scaled_rows * scaled_rows

    def band_mask(lower_cut, upper_cut):
        inside = (radius_sq >= lower_cut * lower_cut) & (radius_sq <= upper_cut * upper_cut)
        return inside.astype(jnp.float32)

    mask_temp = band_mask(band_cuts[0], band_cuts[1])
    mask_pol = band_mask(band_cuts[2], band_cuts[3])
    mask_out = band_mask(band_cuts[4], band_cuts[5])
    radius_floor = jnp.maximum(radius_sq, 1).astype(jnp.float32)
    cos_two = (freq_cols * freq_cols - scaled_rows * scaled_rows).astype(jnp.float32) / radius_floor
    sin_two = (2 * freq_cols * scaled_rows).astype(jnp.float32) / radius_floor
    along_x = (2 * freq_cols).astype(jnp.float32) / NC
    along_y = (2 * freq_rows).astype(jnp.float32) / NR
    spectra = jnp.fft.fft2(sky_maps)
    temp_modes = spectra[0]
    stokes_q = spectra[1]
    stokes_u = spectra[2]
    e_modes = -(cos_two * stokes_q + sin_two * stokes_u)
    b_modes = sin_two * stokes_q - cos_two * stokes_u
    temp_bar = mask_temp * filters[0] * temp_modes
    e_bar = mask_pol * filters[1] * e_modes
    b_bar = mask_pol * filters[2] * b_modes
    rotation = cos_two + 1j * sin_two
    raising = 1j * (along_x + 1j * along_y)
    lowering = 1j * (along_x - 1j * along_y)
    pol_wiener = -(wiener[1] * e_bar) * rotation
    leg_spectra = jnp.stack([
        temp_bar,
        raising * (wiener[0] * temp_bar),
        -(e_bar + 1j * b_bar) * rotation,
        raising * pol_wiener,
        lowering * pol_wiener,
    ])
    leg_maps = jnp.fft.ifft2(leg_spectra)
    current = leg_maps[0] * leg_maps[1] + 0.5 * (jnp.conj(leg_maps[2]) * leg_maps[3] + leg_maps[2] * jnp.conj(leg_maps[4]))
    estimate = jnp.fft.ifft2(mask_out * response * (lowering * jnp.fft.fft2(current)))
    return jnp.stack([jnp.real(estimate), jnp.imag(estimate)]).astype(jnp.float32)
```

```python
import math

import jax
import jax.numpy as jnp
import numpy as np
from jax import lax
from jax.experimental import pallas as pl
from jax.experimental.pallas import tpu as pltpu
from jax.sharding import PartitionSpec as P

LANES = 128
SUBLANES = 8


def high_low(table):
    single = jnp.asarray(table, jnp.float32)
    high = single.astype(jnp.bfloat16)
    low = (single - high.astype(jnp.float32)).astype(jnp.bfloat16)
    return high, low


def host_split(table):
    import ml_dtypes

    single = np.asarray(table, np.float32)
    high = single.astype(ml_dtypes.bfloat16)
    low = (single - high.astype(np.float32)).astype(ml_dtypes.bfloat16)
    return np.stack([high, low])


def unit_circle(left, right, period):
    angles = 2.0 * math.pi / period * (np.outer(left, right) % period)
    return np.cos(angles), np.sin(angles)


def slab_rows(outer, groups, rows_count, fields_count):
    per_source = outer // groups
    source = np.arange(groups)
    block = (source % fields_count) * rows_count + source // fields_count
    return (block[:, None] * per_source + np.arange(per_source)[None, :]).reshape(-1)


def transform_tables(total, scale, groups, rows_count, fields_count):
    outer = total // LANES
    x1 = slab_rows(outer, groups, rows_count, fields_count)
    k1 = np.arange(outer)
    x2 = np.arange(LANES)
    first_cos, first_sin = unit_circle(k1, x1, outer)
    last_cos, last_sin = unit_circle(x2, x2, LANES)
    turn_cos, turn_sin = unit_circle(k1, x2, total)
    forward_left = host_split(np.block([[first_cos, first_sin], [-first_sin, first_cos]]))
    forward_right = host_split(np.block([[last_cos, -last_sin], [last_sin, last_cos]]))
    inverse_right = host_split(np.block([[last_cos, last_sin], [-last_sin, last_cos]]))
    inverse_left = host_split(
        np.block([[first_cos.T, -first_sin.T], [first_sin.T, first_cos.T]])
    )
    turns = np.stack([turn_cos, -turn_sin, turn_cos * scale, turn_sin * scale])
    return forward_left, forward_right, inverse_right, inverse_left, np.asarray(turns, np.float32)


def rotate(cosine, sine, real, imag):
    if imag is None:
        return real * cosine, real * sine
    if abs(cosine - abs(sine)) < 1e-12 or abs(cosine + abs(sine)) < 1e-12:
        sign = 1.0 if cosine * sine > 0 else -1.0
        if sign > 0:
            return (real - imag) * cosine, (real + imag) * cosine
        return (real + imag) * cosine, (imag - real) * cosine
    return real * cosine - imag * sine, real * sine + imag * cosine


def tile_transform(values, direction):
    length = len(values)
    if length == 1:
        return values
    even = tile_transform(values[0::2], direction)
    odd = tile_transform(values[1::2], direction)
    half = length // 2
    low, high = [None] * half, [None] * half
    for index in range(half):
        even_real, even_imag = even[index]
        odd_real, odd_imag = odd[index]
        if index == 0:
            low[0] = (
                even_real + odd_real,
                None if even_imag is None else even_imag + odd_imag,
            )
            high[0] = (
                even_real - odd_real,
                None if even_imag is None else even_imag - odd_imag,
            )
            continue
        if 4 * index == length:
            if odd_imag is None:
                turned_real, turned_imag = None, odd_real
            else:
                turned_real, turned_imag = odd_imag, odd_real
            if direction > 0:
                real_low = even_real if turned_real is None else even_real - turned_real
                real_high = even_real if turned_real is None else even_real + turned_real
                imag_low = turned_imag if even_imag is None else even_imag + turned_imag
                imag_high = -turned_imag if even_imag is None else even_imag - turned_imag
            else:
                real_low = even_real if turned_real is None else even_real + turned_real
                real_high = even_real if turned_real is None else even_real - turned_real
                imag_low = -turned_imag if even_imag is None else even_imag - turned_imag
                imag_high = turned_imag if even_imag is None else even_imag + turned_imag
            low[index] = (real_low, imag_low)
            high[index] = (real_high, imag_high)
            continue
        angle = direction * 2.0 * math.pi * index / length
        turned_real, turned_imag = rotate(math.cos(angle), math.sin(angle), odd_real, odd_imag)
        low[index] = (
            even_real + turned_real,
            turned_imag if even_imag is None else even_imag + turned_imag,
        )
        high[index] = (
            even_real - turned_real,
            -turned_imag if even_imag is None else even_imag - turned_imag,
        )
    return low + high


def split_product_left(table_ref, data):
    high = data.astype(jnp.bfloat16)
    low = (data - high.astype(jnp.float32)).astype(jnp.bfloat16)
    product = lambda a, b: jnp.dot(a, b, preferred_element_type=jnp.float32)
    return product(table_ref[0], high) + product(table_ref[0], low) + product(table_ref[1], high)


def split_product_right(data, table_ref):
    high = data.astype(jnp.bfloat16)
    low = (data - high.astype(jnp.float32)).astype(jnp.bfloat16)
    product = lambda a, b: jnp.dot(a, b, preferred_element_type=jnp.float32)
    return product(high, table_ref[0]) + product(low, table_ref[0]) + product(high, table_ref[1])


def forward_rows(pairs, left_ref, right_ref, turn_ref):
    outer = pairs[0][0].shape[0]
    stacked = jnp.concatenate(
        [
            jnp.concatenate([pair[0] for pair in pairs], axis=1),
            jnp.concatenate([pair[1] for pair in pairs], axis=1),
        ],
        axis=0,
    )
    middle = split_product_left(left_ref, stacked)
    cosine, sine = turn_ref[0], turn_ref[1]
    rows = []
    for index in range(len(pairs)):
        real = middle[:outer, index * LANES : (index + 1) * LANES]
        imag = middle[outer:, index * LANES : (index + 1) * LANES]
        rows.append(
            jnp.concatenate([real * cosine - imag * sine, real * sine + imag * cosine], axis=1)
        )
    result = split_product_right(jnp.concatenate(rows, axis=0), right_ref)
    return [
        (
            result[index * outer : (index + 1) * outer, :LANES],
            result[index * outer : (index + 1) * outer, LANES:],
        )
        for index in range(len(pairs))
    ]


def inverse_rows(pairs, right_ref, left_ref, turn_ref):
    outer = pairs[0][0].shape[0]
    stacked = jnp.concatenate([jnp.concatenate(pair, axis=1) for pair in pairs], axis=0)
    middle = split_product_right(stacked, right_ref)
    cosine, sine = turn_ref[2], turn_ref[3]
    reals, imags = [], []
    for index in range(len(pairs)):
        real = middle[index * outer : (index + 1) * outer, :LANES]
        imag = middle[index * outer : (index + 1) * outer, LANES:]
        reals.append(real * cosine - imag * sine)
        imags.append(real * sine + imag * cosine)
    stacked = jnp.concatenate(
        [jnp.concatenate(reals, axis=1), jnp.concatenate(imags, axis=1)], axis=0
    )
    result = split_product_left(left_ref, stacked)
    return [
        (
            result[:outer, index * LANES : (index + 1) * LANES],
            result[outer:, index * LANES : (index + 1) * LANES],
        )
        for index in range(len(pairs))
    ]


def split_columns_kernel(sky_ref, out_ref):
    parts = out_ref.shape[0]
    fields, _, width = sky_ref.shape
    tiles = width // parts // LANES
    for part in range(parts):
        for field in range(fields):
            for tile in range(tiles):
                start = (part * tiles + tile) * LANES
                place = (field * tiles + tile) * SUBLANES
                out_ref[part, place : place + SUBLANES, :] = sky_ref[field, :, start : start + LANES]


def join_columns_kernel(in_ref, out_ref):
    parts = in_ref.shape[0]
    fields, _, width = out_ref.shape
    tiles = width // parts // LANES
    for part in range(parts):
        for field in range(fields):
            for tile in range(tiles):
                start = (part * tiles + tile) * LANES
                place = (field * tiles + tile) * SUBLANES
                out_ref[field, :, start : start + LANES] = in_ref[part, place : place + SUBLANES, :]


def slab_forward_kernel(local_rows, sky_ref, out_ref):
    parts, height, _ = sky_ref.shape
    fields = height // (SUBLANES * SUBLANES)
    for field in range(fields):
        values = []
        for part in range(parts):
            for row in range(SUBLANES):
                start = field * SUBLANES * SUBLANES + row
                values.append(
                    (sky_ref[part, pl.ds(start, SUBLANES, stride=SUBLANES), :], None)
                )
        for freq, pair in enumerate(tile_transform(values, -1.0)):
            owner, row = divmod(freq, local_rows)
            for side in range(2):
                place = ((field * 2 + side) * local_rows + row) * SUBLANES
                value = pair[side]
                if value is None:
                    value = jnp.zeros_like(pair[0])
                out_ref[owner, place : place + SUBLANES, :] = value


def tile_rows(ref, leg, local_rows):
    values = []
    for owner in range(ref.shape[0]):
        for row in range(local_rows):
            places = [((leg * 2 + side) * local_rows + row) * SUBLANES for side in range(2)]
            values.append(tuple(ref[owner, p : p + SUBLANES, :] for p in places))
    return values


def product_kernel(local_rows, legs_ref, out_ref, pol_ref, sum_ref):
    temp = tile_transform(tile_rows(legs_ref, 0, local_rows), 1.0)
    for index, (real, imag) in enumerate(temp):
        pol_ref[index, 0] = real
        pol_ref[index, 1] = imag
    grad = tile_transform(tile_rows(legs_ref, 1, local_rows), 1.0)
    for index, (real, imag) in enumerate(grad):
        first, second = pol_ref[index, 0], pol_ref[index, 1]
        sum_ref[index, 0] = first * real - second * imag
        sum_ref[index, 1] = first * imag + second * real
    pol = tile_transform(tile_rows(legs_ref, 2, local_rows), 1.0)
    for index, (real, imag) in enumerate(pol):
        pol_ref[index, 0] = real * 0.5
        pol_ref[index, 1] = imag * 0.5
    three = tile_transform(tile_rows(legs_ref, 3, local_rows), 1.0)
    for index, (real, imag) in enumerate(three):
        first, second = pol_ref[index, 0], pol_ref[index, 1]
        sum_ref[index, 0] += first * real + second * imag
        sum_ref[index, 1] += first * imag - second * real
    one = tile_transform(tile_rows(legs_ref, 4, local_rows), 1.0)
    current = []
    for index, (real, imag) in enumerate(one):
        first, second = pol_ref[index, 0], pol_ref[index, 1]
        current.append(
            (
                sum_ref[index, 0] + (first * real + second * imag),
                sum_ref[index, 1] + (second * real - first * imag),
            )
        )
    for freq, pair in enumerate(tile_transform(current, -1.0)):
        owner, row = divmod(freq, local_rows)
        for side in range(2):
            place = (side * local_rows + row) * SUBLANES
            out_ref[owner, place : place + SUBLANES, :] = pair[side]


def slab_inverse_kernel(local_rows, in_ref, out_ref):
    result = tile_transform(tile_rows(in_ref, 0, local_rows), 1.0)
    for row, pair in enumerate(result):
        part, inner = divmod(row, SUBLANES)
        for side in range(2):
            start = side * SUBLANES * SUBLANES + inner
            out_ref[part, pl.ds(start, SUBLANES, stride=SUBLANES), :] = pair[side]


def gathered_matrix(ref, place):
    sources = ref.shape[0]
    return ref[:, place : place + SUBLANES, :].reshape(sources * SUBLANES, LANES)


def frequencies(row_id, outer, total, total_rows):
    column = lax.broadcasted_iota(jnp.int32, (outer, LANES), 0) + outer * lax.broadcasted_iota(
        jnp.int32, (outer, LANES), 1
    )
    freq_col = jnp.where(column < total // 2, column, column - total)
    freq_row = jnp.where(row_id < total_rows // 2, row_id, row_id - total_rows)
    return freq_col, freq_row


def legs_kernel(
    config, cuts_ref, spectra_ref, filters_ref, wiener_ref, fl_ref, fr_ref, ir_ref, il_ref, turn_ref, out_ref
):
    local_rows, total, total_rows = config
    outer = total // LANES
    ratio = total // total_rows
    device = cuts_ref[6]
    for row in range(local_rows):
        pairs = []
        for field in range(3):
            pairs.append(
                tuple(
                    gathered_matrix(spectra_ref, ((field * 2 + side) * local_rows + row) * SUBLANES)
                    for side in range(2)
                )
            )
        temp, stokes_q, stokes_u = forward_rows(pairs, fl_ref, fr_ref, turn_ref)
        freq_col, freq_row = frequencies(device * local_rows + row, outer, total, total_rows)
        scaled = freq_row * ratio
        square = freq_col * freq_col
        radius = square + scaled * scaled
        floor = jnp.maximum(radius, 1).astype(jnp.float32)
        cosine = (square - scaled * scaled).astype(jnp.float32) / floor
        sine = (freq_col * (2 * scaled)).astype(jnp.float32) / floor
        along_x = freq_col.astype(jnp.float32) * (2.0 / total)
        along_y = freq_row.astype(jnp.float32) * (2.0 / total_rows)

        def weight(ref, index):
            return ref[index, pl.ds(row, outer, stride=local_rows), :].T

        def masked(lower, upper, value):
            low, high = cuts_ref[lower], cuts_ref[upper]
            inside = (radius >= low * low) & (radius <= high * high)
            return jnp.where(inside, value, 0.0)

        temp_weight = masked(0, 1, weight(filters_ref, 0))
        e_weight = masked(2, 3, weight(filters_ref, 1))
        b_weight = masked(2, 3, weight(filters_ref, 2))
        temp_bar = (temp_weight * temp[0], temp_weight * temp[1])
        minus_e = tuple(
            e_weight * (cosine * stokes_q[side] + sine * stokes_u[side]) for side in range(2)
        )
        b_bar = tuple(
            b_weight * (sine * stokes_q[side] - cosine * stokes_u[side]) for side in range(2)
        )
        wiener_temp = weight(wiener_ref, 0)
        grad = (wiener_temp * temp_bar[0], wiener_temp * temp_bar[1])
        grad_leg = (
            -(along_y * grad[0]) - along_x * grad[1],
            along_x * grad[0] - along_y * grad[1],
        )
        pol = (minus_e[0] + b_bar[1], minus_e[1] - b_bar[0])
        pol_leg = (pol[0] * cosine - pol[1] * sine, pol[0] * sine + pol[1] * cosine)
        wiener_pol = weight(wiener_ref, 1)
        scaled_e = (wiener_pol * minus_e[0], wiener_pol * minus_e[1])
        spin = (
            scaled_e[0] * cosine - scaled_e[1] * sine,
            scaled_e[0] * sine + scaled_e[1] * cosine,
        )
        across = (-(along_x * spin[1]), along_x * spin[0])
        upward = (along_y * spin[0], along_y * spin[1])
        three_leg = (across[0] - upward[0], across[1] - upward[1])
        one_leg = (across[0] + upward[0], across[1] + upward[1])
        legs = inverse_rows(
            [temp_bar, grad_leg, pol_leg, three_leg, one_leg], ir_ref, il_ref, turn_ref
        )
        for leg, pair in enumerate(legs):
            for side in range(2):
                place = ((leg * 2 + side) * local_rows + row) * SUBLANES
                out_ref[:, place : place + SUBLANES, :] = pair[side].reshape(
                    out_ref.shape[0], SUBLANES, LANES
                )


def estimate_kernel(
    config, cuts_ref, spectra_ref, response_ref, fl_ref, fr_ref, ir_ref, il_ref, turn_ref, out_ref
):
    local_rows, total, total_rows = config
    outer = total // LANES
    ratio = total // total_rows
    device = cuts_ref[6]
    pairs = [
        tuple(
            gathered_matrix(spectra_ref, (side * local_rows + row) * SUBLANES) for side in range(2)
        )
        for row in range(local_rows)
    ]
    modes = forward_rows(pairs, fl_ref, fr_ref, turn_ref)
    estimates = []
    for row in range(local_rows):
        freq_col, freq_row = frequencies(device * local_rows + row, outer, total, total_rows)
        scaled = freq_row * ratio
        radius = freq_col * freq_col + scaled * scaled
        low, high = cuts_ref[4], cuts_ref[5]
        inside = (radius >= low * low) & (radius <= high * high)
        weight = jnp.where(inside, response_ref[pl.ds(row, outer, stride=local_rows), :].T, 0.0)
        along_x = freq_col.astype(jnp.float32) * (2.0 / total)
        along_y = freq_row.astype(jnp.float32) * (2.0 / total_rows)
        real, imag = weight * modes[row][0], weight * modes[row][1]
        estimates.append(
            (along_y * real - along_x * imag, along_y * imag + along_x * real)
        )
    result = inverse_rows(estimates, ir_ref, il_ref, turn_ref)
    for row in range(local_rows):
        for side in range(2):
            place = (side * local_rows + row) * SUBLANES
            out_ref[:, place : place + SUBLANES, :] = result[row][side].reshape(
                out_ref.shape[0], SUBLANES, LANES
            )


def in_vmem(count):
    return [pl.BlockSpec(memory_space=pltpu.VMEM)] * count


def run(kernel, shape, *operands, scalars=0, scratch=()):
    specs = [pl.BlockSpec(memory_space=pltpu.SMEM)] * scalars + in_vmem(len(operands) - scalars)
    return pl.pallas_call(
        kernel,
        out_shape=jax.ShapeDtypeStruct(shape, jnp.float32),
        in_specs=specs,
        out_specs=pl.BlockSpec(memory_space=pltpu.VMEM),
        scratch_shapes=list(scratch),
        compiler_params=pltpu.CompilerParams(vmem_limit_bytes=48 * 1024 * 1024),
    )(*operands)


def lane_view(table, outer, local_rows):
    lead = table.shape[:-2]
    shaped = table.reshape(lead + (local_rows, outer, LANES))
    order = tuple(range(len(lead))) + (len(lead) + 1, len(lead), len(lead) + 2)
    return shaped.transpose(order).reshape(lead + (outer * local_rows, LANES))


def tiled_body(sky_maps, band_cuts, filters, wiener, response):
    rows_count = lax.axis_size("rows")
    fields_count = lax.axis_size("fields")
    both = ("rows", "fields")
    groups = rows_count * fields_count
    local_rows, total = filters.shape[1:]
    total_rows = local_rows * groups
    outer = total // LANES
    config = (local_rows, total, total_rows)
    scale = 1.0 / (total * total_rows)
    tables = transform_tables(total, scale, groups, rows_count, fields_count)
    device = lax.axis_index(both).astype(jnp.int32)
    cuts = jnp.concatenate([band_cuts, device[None]])
    square = SUBLANES * SUBLANES

    def exchange(value, axes):
        return lax.all_to_all(value, axes, 0, 0, tiled=True)

    pieces = run(split_columns_kernel, (rows_count, 3 * square, LANES), sky_maps)
    slabs = exchange(pieces, "rows")
    spectra = run(
        lambda *refs: slab_forward_kernel(local_rows, *refs),
        (groups, 6 * local_rows * SUBLANES, LANES),
        slabs,
    )
    spectra = exchange(spectra, both)
    legs = run(
        lambda *refs: legs_kernel(config, *refs),
        (groups, 10 * local_rows * SUBLANES, LANES),
        cuts,
        spectra,
        lane_view(filters, outer, local_rows),
        lane_view(wiener, outer, local_rows),
        *tables,
        scalars=1,
    )
    legs = exchange(legs, both)
    holder = pltpu.VMEM((total_rows, 2, SUBLANES, LANES), jnp.float32)
    current = run(
        lambda *refs: product_kernel(local_rows, *refs),
        (groups, 2 * local_rows * SUBLANES, LANES),
        legs,
        scratch=(holder, holder),
    )
    current = exchange(current, both)
    estimate = run(
        lambda *refs: estimate_kernel(config, *refs),
        (groups, 2 * local_rows * SUBLANES, LANES),
        cuts,
        current,
        lane_view(response, outer, local_rows),
        *tables,
        scalars=1,
    )
    estimate = exchange(estimate, both)
    maps = run(
        lambda *refs: slab_inverse_kernel(local_rows, *refs),
        (rows_count, 2 * square, LANES),
        estimate,
    )
    maps = exchange(maps, "rows")
    return run(join_columns_kernel, (2, SUBLANES, sky_maps.shape[2]), maps)


exact_mode = lax.Precision.HIGHEST


def split_factor(length):
    best_first = 1
    for divisor in range(1, math.isqrt(length) + 1):
        if length % divisor == 0:
            best_first = divisor
    return (best_first, length // best_first)


def phase_table(left_index, right_index, period, direction):
    product = left_index[:, None] * right_index[None, :] % period
    angles = direction * 2.0 * math.pi / period * product.astype(jnp.float32)
    return (jnp.cos(angles), jnp.sin(angles))


def complex_einsum(formula, data_pair, table_pair):
    data_real, data_imag = data_pair
    table_real, table_imag = table_pair
    real_out = jnp.einsum(formula, data_real, table_real, precision=exact_mode)
    imag_out = jnp.einsum(formula, data_real, table_imag, precision=exact_mode)
    if data_imag is not None:
        real_out = real_out - jnp.einsum(formula, data_imag, table_imag, precision=exact_mode)
        imag_out = imag_out + jnp.einsum(formula, data_imag, table_real, precision=exact_mode)
    return (real_out, imag_out)


def complex_mul(left_pair, right_pair):
    return (
        left_pair[0] * right_pair[0] - left_pair[1] * right_pair[1],
        left_pair[0] * right_pair[1] + left_pair[1] * right_pair[0],
    )


def conj_mul(left_pair, right_pair):
    return (
        left_pair[0] * right_pair[0] + left_pair[1] * right_pair[1],
        left_pair[0] * right_pair[1] - left_pair[1] * right_pair[0],
    )


def row_transform(data_pair, direction):
    batch_len, length, block_width = data_pair[0].shape
    outer_len, inner_len = split_factor(length)
    outer_ids = jnp.arange(outer_len, dtype=jnp.int32)
    inner_ids = jnp.arange(inner_len, dtype=jnp.int32)
    real_in = data_pair[0].reshape(batch_len, outer_len, inner_len, block_width)
    imag_in = None
    if data_pair[1] is not None:
        imag_in = data_pair[1].reshape(batch_len, outer_len, inner_len, block_width)
    middle = complex_einsum(
        "bjmc,jk->bkmc", (real_in, imag_in), phase_table(outer_ids, outer_ids, outer_len, direction)
    )
    twiddle = phase_table(outer_ids, inner_ids, length, direction)
    middle = complex_mul(middle, (twiddle[0][None, :, :, None], twiddle[1][None, :, :, None]))
    result = complex_einsum(
        "bkmc,mq->bqkc", middle, phase_table(inner_ids, inner_ids, inner_len, direction)
    )
    norm_factor = 1.0 if direction < 0 else 1.0 / length
    return (
        result[0].reshape(batch_len, length, block_width) * norm_factor,
        result[1].reshape(batch_len, length, block_width) * norm_factor,
    )


def block_order(groups, fields_count):
    positions = jnp.arange(groups, dtype=jnp.int32)
    blocks = positions % fields_count * (groups // fields_count) + positions // fields_count
    return (positions, blocks)


def column_forward(data_pair, groups, fields_count):
    batch_len, local_rows, total_len = data_pair[0].shape
    block_width = total_len // groups
    positions, blocks = block_order(groups, fields_count)
    column_ids = jnp.arange(block_width, dtype=jnp.int32)
    shaped = (
        data_pair[0].reshape(batch_len, local_rows, groups, block_width),
        data_pair[1].reshape(batch_len, local_rows, groups, block_width),
    )
    middle = complex_einsum("brpc,pk->brkc", shaped, phase_table(blocks, positions, groups, -1.0))
    twiddle = phase_table(positions, column_ids, total_len, -1.0)
    middle = complex_mul(middle, (twiddle[0][None, None], twiddle[1][None, None]))
    result = complex_einsum(
        "brkc,cq->brqk", middle, phase_table(column_ids, column_ids, block_width, -1.0)
    )
    return (
        result[0].reshape(batch_len, local_rows, total_len),
        result[1].reshape(batch_len, local_rows, total_len),
    )


def column_inverse(data_pair, groups, fields_count):
    batch_len, local_rows, total_len = data_pair[0].shape
    block_width = total_len // groups
    positions, blocks = block_order(groups, fields_count)
    column_ids = jnp.arange(block_width, dtype=jnp.int32)
    shaped = (
        data_pair[0].reshape(batch_len, local_rows, block_width, groups),
        data_pair[1].reshape(batch_len, local_rows, block_width, groups),
    )
    middle = complex_einsum(
        "brqk,qc->brkc", shaped, phase_table(column_ids, column_ids, block_width, 1.0)
    )
    twiddle = phase_table(positions, column_ids, total_len, 1.0)
    middle = complex_mul(middle, (twiddle[0][None, None], twiddle[1][None, None]))
    result = complex_einsum("brkc,kp->brpc", middle, phase_table(positions, blocks, groups, 1.0))
    norm_factor = 1.0 / total_len
    return (
        result[0].reshape(batch_len, local_rows, total_len) * norm_factor,
        result[1].reshape(batch_len, local_rows, total_len) * norm_factor,
    )


def general_body(sky_maps, band_cuts, filters, wiener, response):
    rows_count = lax.axis_size("rows")
    fields_count = lax.axis_size("fields")
    groups = rows_count * fields_count
    local_rows = filters.shape[1]
    total_rows = local_rows * groups
    NC = filters.shape[2]
    row_ratio = NC // total_rows

    def forward_columns(stacked):
        return jnp.stack(column_forward((stacked[0], stacked[1]), groups, fields_count))

    def inverse_slabs(stacked):
        return jnp.stack(row_transform((stacked[0], stacked[1]), 1.0))

    def inverse_columns(stacked):
        return jnp.stack(column_inverse((stacked[0], stacked[1]), groups, fields_count))

    def to_frequency(stacked):
        batch_len = stacked.shape[1]
        block_width = stacked.shape[3]
        shaped = stacked.reshape(
            2, batch_len, rows_count, fields_count, local_rows, 1, 1, block_width
        )
        arrived = lax.all_to_all(
            lax.all_to_all(shaped, "rows", split_axis=2, concat_axis=5, tiled=True),
            "fields",
            split_axis=3,
            concat_axis=6,
            tiled=True,
        )
        result = forward_columns(arrived.reshape(2, batch_len, local_rows, groups * block_width))
        return result

    def to_space(stacked):
        batch_len = stacked.shape[1]
        block_width = stacked.shape[3] // groups
        shaped = stacked.reshape(
            2, batch_len, 1, 1, local_rows, rows_count, fields_count, block_width
        )
        arrived = lax.all_to_all(
            lax.all_to_all(shaped, "rows", split_axis=5, concat_axis=2, tiled=True),
            "fields",
            split_axis=6,
            concat_axis=3,
            tiled=True,
        )
        result = inverse_slabs(arrived.reshape(2, batch_len, total_rows, block_width))
        return result

    slab_spectra = jnp.stack(
        row_transform(
            (lax.all_to_all(sky_maps, "rows", split_axis=2, concat_axis=1, tiled=True), None), -1.0
        )
    )
    sky_spectra = to_frequency(slab_spectra)
    row_ids = lax.axis_index(("rows", "fields")) * local_rows + jnp.arange(
        local_rows, dtype=jnp.int32
    )
    freq_rows = jnp.where(row_ids < total_rows // 2, row_ids, row_ids - total_rows)[:, None]
    column_ids = jnp.arange(NC, dtype=jnp.int32)
    freq_cols = jnp.where(column_ids < NC // 2, column_ids, column_ids - NC)[None, :]
    scaled_rows = row_ratio * freq_rows
    radius_sq = freq_cols * freq_cols + scaled_rows * scaled_rows

    def band_mask(lower_cut, upper_cut):
        inside = (radius_sq >= lower_cut * lower_cut) & (radius_sq <= upper_cut * upper_cut)
        return inside.astype(jnp.float32)

    mask_temp = band_mask(band_cuts[0], band_cuts[1])
    mask_pol = band_mask(band_cuts[2], band_cuts[3])
    mask_out = band_mask(band_cuts[4], band_cuts[5])
    radius_floor = jnp.maximum(radius_sq, 1).astype(jnp.float32)
    cos_two = (freq_cols * freq_cols - scaled_rows * scaled_rows).astype(jnp.float32) / radius_floor
    sin_two = (2 * freq_cols * scaled_rows).astype(jnp.float32) / radius_floor
    along_x = (2 * freq_cols).astype(jnp.float32) / NC
    along_y = (2 * freq_rows).astype(jnp.float32) / total_rows
    raising = (-along_y + 0.0 * along_x, along_x + 0.0 * along_y)
    lowering = (along_y + 0.0 * along_x, along_x + 0.0 * along_y)
    rotation = (cos_two, sin_two)
    temp_modes = (sky_spectra[0, 0], sky_spectra[1, 0])
    stokes_q = (sky_spectra[0, 1], sky_spectra[1, 1])
    stokes_u = (sky_spectra[0, 2], sky_spectra[1, 2])
    e_modes = (
        -(cos_two * stokes_q[0] + sin_two * stokes_u[0]),
        -(cos_two * stokes_q[1] + sin_two * stokes_u[1]),
    )
    b_modes = (
        sin_two * stokes_q[0] - cos_two * stokes_u[0],
        sin_two * stokes_q[1] - cos_two * stokes_u[1],
    )
    temp_weight = mask_temp * filters[0]
    e_weight = mask_pol * filters[1]
    b_weight = mask_pol * filters[2]
    temp_bar = (temp_weight * temp_modes[0], temp_weight * temp_modes[1])
    e_bar = (e_weight * e_modes[0], e_weight * e_modes[1])
    b_bar = (b_weight * b_modes[0], b_weight * b_modes[1])
    grad_temp = complex_mul(raising, (wiener[0] * temp_bar[0], wiener[0] * temp_bar[1]))
    pol_sum = complex_mul((e_bar[0] - b_bar[1], e_bar[1] + b_bar[0]), rotation)
    pol_bar = (-pol_sum[0], -pol_sum[1])
    pol_rot = complex_mul((wiener[1] * e_bar[0], wiener[1] * e_bar[1]), rotation)
    pol_wiener = (-pol_rot[0], -pol_rot[1])
    spin_three = complex_mul(raising, pol_wiener)
    spin_one = complex_mul(lowering, pol_wiener)
    leg_spectra = jnp.stack(
        [
            jnp.stack([temp_bar[0], grad_temp[0], pol_bar[0], spin_three[0], spin_one[0]]),
            jnp.stack([temp_bar[1], grad_temp[1], pol_bar[1], spin_three[1], spin_one[1]]),
        ]
    )
    leg_maps = to_space(inverse_columns(leg_spectra))
    temp_leg = (leg_maps[0, 0], leg_maps[1, 0])
    grad_leg = (leg_maps[0, 1], leg_maps[1, 1])
    pol_leg = (leg_maps[0, 2], leg_maps[1, 2])
    three_leg = (leg_maps[0, 3], leg_maps[1, 3])
    one_leg = (leg_maps[0, 4], leg_maps[1, 4])
    temp_term = complex_mul(temp_leg, grad_leg)
    raise_term = conj_mul(pol_leg, three_leg)
    lower_term = conj_mul(one_leg, pol_leg)
    current = (
        temp_term[0] + 0.5 * (raise_term[0] + lower_term[0]),
        temp_term[1] + 0.5 * (raise_term[1] + lower_term[1]),
    )
    current_rows = jnp.stack(row_transform((current[0][None], current[1][None]), -1.0))
    current_modes = to_frequency(current_rows)
    out_weight = mask_out * response
    estimate_modes = complex_mul(
        lowering, (out_weight * current_modes[0, 0], out_weight * current_modes[1, 0])
    )
    estimate_stack = jnp.stack([estimate_modes[0][None], estimate_modes[1][None]])
    estimate_maps = to_space(inverse_columns(estimate_stack))
    slab_result = estimate_maps[:, 0]
    return lax.all_to_all(slab_result, "rows", split_axis=1, concat_axis=2, tiled=True)


def fits_tiles(sky_maps, band_cuts, filters, wiener, response):
    groups = lax.axis_size("rows") * lax.axis_size("fields")
    return (
        sky_maps.shape[1] == SUBLANES
        and filters.shape[2] // groups == SUBLANES * LANES
        and filters.shape[2] == LANES * LANES
    )


def body(*operands):
    return tiled_body(*operands) if fits_tiles(*operands) else general_body(*operands)


def solution(mesh):
    placed = (
        P("sims", "rows", "fields"),
        P(),
        P(None, ("rows", "fields"), None),
        P(None, ("rows", "fields"), None),
        P(("rows", "fields"), None),
    )
    return jax.shard_map(
        body, mesh=mesh, in_specs=placed, out_specs=P("sims", "rows", "fields"), check_vma=False
    )
```

```python
import math

import jax
import jax.numpy as jnp
import numpy as np
from jax import lax
from jax.experimental import pallas as pl
from jax.experimental.pallas import tpu as pltpu
from jax.sharding import PartitionSpec as P

LANES = 128
SUBLANES = 8


def host_split(table):
    import ml_dtypes

    single = np.asarray(table, np.float32)
    high = single.astype(ml_dtypes.bfloat16)
    low = (single - high.astype(np.float32)).astype(ml_dtypes.bfloat16)
    return np.stack([high, low])


def unit_circle(left, right, period):
    angles = 2.0 * math.pi / period * (np.outer(left, right) % period)
    return np.cos(angles), np.sin(angles)


def slab_rows(outer, groups, rows_count, fields_count):
    per_source = outer // groups
    source = np.arange(groups)
    block = (source % fields_count) * rows_count + source // fields_count
    return (block[:, None] * per_source + np.arange(per_source)[None, :]).reshape(-1)


def transform_tables(total, scale, groups, rows_count, fields_count):
    outer = total // LANES
    x1 = slab_rows(outer, groups, rows_count, fields_count)
    k1 = np.arange(outer)
    x2 = np.arange(LANES)
    first_cos, first_sin = unit_circle(k1, x1, outer)
    last_cos, last_sin = unit_circle(x2, x2, LANES)
    turn_cos, turn_sin = unit_circle(k1, x2, total)
    forward_left = host_split(np.block([[first_cos, first_sin], [-first_sin, first_cos]]))
    forward_right = host_split(np.block([[last_cos, -last_sin], [last_sin, last_cos]]))
    inverse_right = host_split(np.block([[last_cos, last_sin], [-last_sin, last_cos]]))
    inverse_left = host_split(
        np.block([[first_cos.T, -first_sin.T], [first_sin.T, first_cos.T]])
    )
    turns = np.stack([turn_cos, -turn_sin, turn_cos * scale, turn_sin * scale])
    return forward_left, forward_right, inverse_right, inverse_left, np.asarray(turns, np.float32)


def rotate(cosine, sine, real, imag):
    if imag is None:
        return real * cosine, real * sine
    if abs(cosine - abs(sine)) < 1e-12 or abs(cosine + abs(sine)) < 1e-12:
        sign = 1.0 if cosine * sine > 0 else -1.0
        if sign > 0:
            return (real - imag) * cosine, (real + imag) * cosine
        return (real + imag) * cosine, (imag - real) * cosine
    return real * cosine - imag * sine, real * sine + imag * cosine


def tile_transform(values, direction):
    length = len(values)
    if length == 1:
        return values
    even = tile_transform(values[0::2], direction)
    odd = tile_transform(values[1::2], direction)
    half = length // 2
    low, high = [None] * half, [None] * half
    for index in range(half):
        even_real, even_imag = even[index]
        odd_real, odd_imag = odd[index]
        if index == 0:
            low[0] = (
                even_real + odd_real,
                None if even_imag is None else even_imag + odd_imag,
            )
            high[0] = (
                even_real - odd_real,
                None if even_imag is None else even_imag - odd_imag,
            )
            continue
        if 4 * index == length:
            if odd_imag is None:
                turned_real, turned_imag = None, odd_real
            else:
                turned_real, turned_imag = odd_imag, odd_real
            if direction > 0:
                real_low = even_real if turned_real is None else even_real - turned_real
                real_high = even_real if turned_real is None else even_real + turned_real
                imag_low = turned_imag if even_imag is None else even_imag + turned_imag
                imag_high = -turned_imag if even_imag is None else even_imag - turned_imag
            else:
                real_low = even_real if turned_real is None else even_real + turned_real
                real_high = even_real if turned_real is None else even_real - turned_real
                imag_low = -turned_imag if even_imag is None else even_imag - turned_imag
                imag_high = turned_imag if even_imag is None else even_imag + turned_imag
            low[index] = (real_low, imag_low)
            high[index] = (real_high, imag_high)
            continue
        angle = direction * 2.0 * math.pi * index / length
        turned_real, turned_imag = rotate(math.cos(angle), math.sin(angle), odd_real, odd_imag)
        low[index] = (
            even_real + turned_real,
            turned_imag if even_imag is None else even_imag + turned_imag,
        )
        high[index] = (
            even_real - turned_real,
            -turned_imag if even_imag is None else even_imag - turned_imag,
        )
    return low + high


def split_product_left(table_ref, data):
    high = data.astype(jnp.bfloat16)
    low = (data - high.astype(jnp.float32)).astype(jnp.bfloat16)
    product = lambda a, b: jnp.dot(a, b, preferred_element_type=jnp.float32)
    return product(table_ref[0], high) + product(table_ref[0], low) + product(table_ref[1], high)


def split_product_right(data, table_ref):
    high = data.astype(jnp.bfloat16)
    low = (data - high.astype(jnp.float32)).astype(jnp.bfloat16)
    product = lambda a, b: jnp.dot(a, b, preferred_element_type=jnp.float32)
    return product(high, table_ref[0]) + product(low, table_ref[0]) + product(high, table_ref[1])


def forward_rows(pairs, left_ref, right_ref, turn_ref):
    outer = pairs[0][0].shape[0]
    stacked = jnp.concatenate(
        [
            jnp.concatenate([pair[0] for pair in pairs], axis=1),
            jnp.concatenate([pair[1] for pair in pairs], axis=1),
        ],
        axis=0,
    )
    middle = split_product_left(left_ref, stacked)
    cosine, sine = turn_ref[0], turn_ref[1]
    rows = []
    for index in range(len(pairs)):
        real = middle[:outer, index * LANES : (index + 1) * LANES]
        imag = middle[outer:, index * LANES : (index + 1) * LANES]
        rows.append(
            jnp.concatenate([real * cosine - imag * sine, real * sine + imag * cosine], axis=1)
        )
    result = split_product_right(jnp.concatenate(rows, axis=0), right_ref)
    return [
        (
            result[index * outer : (index + 1) * outer, :LANES],
            result[index * outer : (index + 1) * outer, LANES:],
        )
        for index in range(len(pairs))
    ]


def inverse_rows(pairs, right_ref, left_ref, turn_ref):
    outer = pairs[0][0].shape[0]
    stacked = jnp.concatenate([jnp.concatenate(pair, axis=1) for pair in pairs], axis=0)
    middle = split_product_right(stacked, right_ref)
    cosine, sine = turn_ref[2], turn_ref[3]
    reals, imags = [], []
    for index in range(len(pairs)):
        real = middle[index * outer : (index + 1) * outer, :LANES]
        imag = middle[index * outer : (index + 1) * outer, LANES:]
        reals.append(real * cosine - imag * sine)
        imags.append(real * sine + imag * cosine)
    stacked = jnp.concatenate(
        [jnp.concatenate(reals, axis=1), jnp.concatenate(imags, axis=1)], axis=0
    )
    result = split_product_left(left_ref, stacked)
    return [
        (
            result[:outer, index * LANES : (index + 1) * LANES],
            result[outer:, index * LANES : (index + 1) * LANES],
        )
        for index in range(len(pairs))
    ]


def split_columns_kernel(sky_ref, *out_refs):
    parts = len(out_refs)
    fields, _, width = sky_ref.shape
    tiles = width // parts // LANES
    for flip in range(parts):
        part = lax.axis_index("rows") ^ flip
        for field in range(fields):
            for tile in range(tiles):
                start = pl.multiple_of((part * tiles + tile) * LANES, LANES)
                place = (field * tiles + tile) * SUBLANES
                out_refs[flip][place : place + SUBLANES, :] = sky_ref[field, :, pl.ds(start, LANES)]


def join_columns_kernel(*refs):
    in_refs, out_ref = refs[:-1], refs[-1]
    parts = len(in_refs)
    fields, _, width = out_ref.shape
    tiles = width // parts // LANES
    for flip in range(parts):
        part = lax.axis_index("rows") ^ flip
        for field in range(fields):
            for tile in range(tiles):
                start = pl.multiple_of((part * tiles + tile) * LANES, LANES)
                place = (field * tiles + tile) * SUBLANES
                out_ref[field, :, pl.ds(start, LANES)] = in_refs[flip][place : place + SUBLANES, :]


def slab_forward_kernel(local_rows, *refs):
    piece_refs, out_ref, sky_ref = refs[:-2], refs[-2], refs[-1]
    for flip, piece_ref in enumerate(piece_refs):
        sky_ref[lax.axis_index("rows") ^ flip] = piece_ref[...]
    parts, height, _ = sky_ref.shape
    fields = height // (SUBLANES * SUBLANES)
    for field in range(fields):
        values = []
        for part in range(parts):
            for row in range(SUBLANES):
                start = field * SUBLANES * SUBLANES + row
                values.append(
                    (sky_ref[part, pl.ds(start, SUBLANES, stride=SUBLANES), :], None)
                )
        for freq, pair in enumerate(tile_transform(values, -1.0)):
            owner, row = divmod(freq, local_rows)
            for side in range(2):
                place = ((field * 2 + side) * local_rows + row) * SUBLANES
                value = pair[side]
                if value is None:
                    value = jnp.zeros_like(pair[0])
                out_ref[owner, place : place + SUBLANES, :] = value


def tile_rows(ref, leg, local_rows):
    values = []
    for owner in range(ref.shape[0]):
        for row in range(local_rows):
            places = [((leg * 2 + side) * local_rows + row) * SUBLANES for side in range(2)]
            values.append(tuple(ref[owner, p : p + SUBLANES, :] for p in places))
    return values


def product_kernel(local_rows, legs_ref, out_ref, pol_ref, sum_ref):
    temp = tile_transform(tile_rows(legs_ref, 0, local_rows), 1.0)
    for index, (real, imag) in enumerate(temp):
        pol_ref[index, 0] = real
        pol_ref[index, 1] = imag
    grad = tile_transform(tile_rows(legs_ref, 1, local_rows), 1.0)
    for index, (real, imag) in enumerate(grad):
        first, second = pol_ref[index, 0], pol_ref[index, 1]
        sum_ref[index, 0] = first * real - second * imag
        sum_ref[index, 1] = first * imag + second * real
    pol = tile_transform(tile_rows(legs_ref, 2, local_rows), 1.0)
    for index, (real, imag) in enumerate(pol):
        pol_ref[index, 0] = real * 0.5
        pol_ref[index, 1] = imag * 0.5
    three = tile_transform(tile_rows(legs_ref, 3, local_rows), 1.0)
    for index, (real, imag) in enumerate(three):
        first, second = pol_ref[index, 0], pol_ref[index, 1]
        sum_ref[index, 0] += first * real + second * imag
        sum_ref[index, 1] += first * imag - second * real
    one = tile_transform(tile_rows(legs_ref, 4, local_rows), 1.0)
    current = []
    for index, (real, imag) in enumerate(one):
        first, second = pol_ref[index, 0], pol_ref[index, 1]
        current.append(
            (
                sum_ref[index, 0] + (first * real + second * imag),
                sum_ref[index, 1] + (second * real - first * imag),
            )
        )
    for freq, pair in enumerate(tile_transform(current, -1.0)):
        owner, row = divmod(freq, local_rows)
        for side in range(2):
            place = (side * local_rows + row) * SUBLANES
            out_ref[owner, place : place + SUBLANES, :] = pair[side]


def slab_inverse_kernel(local_rows, in_ref, *refs):
    out_refs, map_ref = refs[:-1], refs[-1]
    result = tile_transform(tile_rows(in_ref, 0, local_rows), 1.0)
    for row, pair in enumerate(result):
        part, inner = divmod(row, SUBLANES)
        for side in range(2):
            start = side * SUBLANES * SUBLANES + inner
            map_ref[part, pl.ds(start, SUBLANES, stride=SUBLANES), :] = pair[side]
    for flip, out_ref in enumerate(out_refs):
        out_ref[...] = map_ref[lax.axis_index("rows") ^ flip]


def gathered_matrix(ref, place):
    sources = ref.shape[0]
    return ref[:, place : place + SUBLANES, :].reshape(sources * SUBLANES, LANES)


def frequencies(row_id, outer, total, total_rows):
    column = lax.broadcasted_iota(jnp.int32, (outer, LANES), 0) + outer * lax.broadcasted_iota(
        jnp.int32, (outer, LANES), 1
    )
    freq_col = jnp.where(column < total // 2, column, column - total)
    freq_row = jnp.where(row_id < total_rows // 2, row_id, row_id - total_rows)
    return freq_col, freq_row


def legs_kernel(
    config, cuts_ref, spectra_ref, filters_ref, wiener_ref, fl_ref, fr_ref, ir_ref, il_ref, turn_ref, out_ref
):
    local_rows, total, total_rows = config
    outer = total // LANES
    ratio = total // total_rows
    device = lax.axis_index(("rows", "fields"))
    squares = [cuts_ref[cut : cut + 1, :] * cuts_ref[cut : cut + 1, :] for cut in range(4)]
    for row in range(local_rows):
        pairs = []
        for field in range(3):
            pairs.append(
                tuple(
                    gathered_matrix(spectra_ref, ((field * 2 + side) * local_rows + row) * SUBLANES)
                    for side in range(2)
                )
            )
        temp, stokes_q, stokes_u = forward_rows(pairs, fl_ref, fr_ref, turn_ref)
        freq_col, freq_row = frequencies(device * local_rows + row, outer, total, total_rows)
        scaled = freq_row * ratio
        square = freq_col * freq_col
        radius = square + scaled * scaled
        floor = jnp.maximum(radius, 1).astype(jnp.float32)
        cosine = (square - scaled * scaled).astype(jnp.float32) / floor
        sine = (freq_col * (2 * scaled)).astype(jnp.float32) / floor
        along_x = freq_col.astype(jnp.float32) * (2.0 / total)
        along_y = freq_row.astype(jnp.float32) * (2.0 / total_rows)

        def weight(ref, index):
            return ref[index, pl.ds(row, outer, stride=local_rows), :].T

        def masked(lower, upper, value):
            inside = (radius >= squares[lower]) & (radius <= squares[upper])
            return jnp.where(inside, value, 0.0)

        temp_weight = masked(0, 1, weight(filters_ref, 0))
        e_weight = masked(2, 3, weight(filters_ref, 1))
        b_weight = masked(2, 3, weight(filters_ref, 2))
        temp_bar = (temp_weight * temp[0], temp_weight * temp[1])
        minus_e = tuple(
            e_weight * (cosine * stokes_q[side] + sine * stokes_u[side]) for side in range(2)
        )
        b_bar = tuple(
            b_weight * (sine * stokes_q[side] - cosine * stokes_u[side]) for side in range(2)
        )
        wiener_temp = weight(wiener_ref, 0)
        grad = (wiener_temp * temp_bar[0], wiener_temp * temp_bar[1])
        grad_leg = (
            -(along_y * grad[0]) - along_x * grad[1],
            along_x * grad[0] - along_y * grad[1],
        )
        pol = (minus_e[0] + b_bar[1], minus_e[1] - b_bar[0])
        pol_leg = (pol[0] * cosine - pol[1] * sine, pol[0] * sine + pol[1] * cosine)
        wiener_pol = weight(wiener_ref, 1)
        scaled_e = (wiener_pol * minus_e[0], wiener_pol * minus_e[1])
        spin = (
            scaled_e[0] * cosine - scaled_e[1] * sine,
            scaled_e[0] * sine + scaled_e[1] * cosine,
        )
        across = (-(along_x * spin[1]), along_x * spin[0])
        upward = (along_y * spin[0], along_y * spin[1])
        three_leg = (across[0] - upward[0], across[1] - upward[1])
        one_leg = (across[0] + upward[0], across[1] + upward[1])
        legs = inverse_rows(
            [temp_bar, grad_leg, pol_leg, three_leg, one_leg], ir_ref, il_ref, turn_ref
        )
        for leg, pair in enumerate(legs):
            for side in range(2):
                place = ((leg * 2 + side) * local_rows + row) * SUBLANES
                out_ref[:, place : place + SUBLANES, :] = pair[side].reshape(
                    out_ref.shape[0], SUBLANES, LANES
                )


def estimate_kernel(
    config, cuts_ref, spectra_ref, response_ref, fl_ref, fr_ref, ir_ref, il_ref, turn_ref, out_ref
):
    local_rows, total, total_rows = config
    outer = total // LANES
    ratio = total // total_rows
    device = lax.axis_index(("rows", "fields"))
    pairs = [
        tuple(
            gathered_matrix(spectra_ref, (side * local_rows + row) * SUBLANES) for side in range(2)
        )
        for row in range(local_rows)
    ]
    modes = forward_rows(pairs, fl_ref, fr_ref, turn_ref)
    estimates = []
    squares = [cuts_ref[cut : cut + 1, :] * cuts_ref[cut : cut + 1, :] for cut in (4, 5)]
    for row in range(local_rows):
        freq_col, freq_row = frequencies(device * local_rows + row, outer, total, total_rows)
        scaled = freq_row * ratio
        radius = freq_col * freq_col + scaled * scaled
        inside = (radius >= squares[0]) & (radius <= squares[1])
        weight = jnp.where(inside, response_ref[pl.ds(row, outer, stride=local_rows), :].T, 0.0)
        along_x = freq_col.astype(jnp.float32) * (2.0 / total)
        along_y = freq_row.astype(jnp.float32) * (2.0 / total_rows)
        real, imag = weight * modes[row][0], weight * modes[row][1]
        estimates.append(
            (along_y * real - along_x * imag, along_y * imag + along_x * real)
        )
    result = inverse_rows(estimates, ir_ref, il_ref, turn_ref)
    for row in range(local_rows):
        for side in range(2):
            place = (side * local_rows + row) * SUBLANES
            out_ref[:, place : place + SUBLANES, :] = result[row][side].reshape(
                out_ref.shape[0], SUBLANES, LANES
            )


def run(kernel, shape, *operands, scratch=(), copies=None):
    result = jax.ShapeDtypeStruct(shape, jnp.float32)
    place = pl.BlockSpec(memory_space=pltpu.VMEM)
    return pl.pallas_call(
        kernel,
        out_shape=result if copies is None else [result] * copies,
        in_specs=[place] * len(operands),
        out_specs=place if copies is None else [place] * copies,
        scratch_shapes=list(scratch),
        compiler_params=pltpu.CompilerParams(vmem_limit_bytes=48 * 1024 * 1024),
    )(*operands)


def exchange_pieces(pieces, axis):
    count = len(pieces)
    return [pieces[0]] + [
        lax.ppermute(pieces[flip], axis, [(index, index ^ flip) for index in range(count)])
        for flip in range(1, count)
    ]


def lane_view(table, outer, local_rows):
    lead = table.shape[:-2]
    shaped = table.reshape(lead + (local_rows, outer, LANES))
    order = tuple(range(len(lead))) + (len(lead) + 1, len(lead), len(lead) + 2)
    return shaped.transpose(order).reshape(lead + (outer * local_rows, LANES))


def tiled_body(sky_maps, band_cuts, filters, wiener, response):
    rows_count = lax.axis_size("rows")
    fields_count = lax.axis_size("fields")
    both = ("rows", "fields")
    groups = rows_count * fields_count
    local_rows, total = filters.shape[1:]
    total_rows = local_rows * groups
    outer = total // LANES
    config = (local_rows, total, total_rows)
    scale = 1.0 / (total * total_rows)
    tables = transform_tables(total, scale, groups, rows_count, fields_count)
    cuts = jnp.broadcast_to(
        jnp.pad(band_cuts, (0, SUBLANES - band_cuts.shape[0]))[:, None], (SUBLANES, LANES)
    )
    square = SUBLANES * SUBLANES

    def exchange(value, axes):
        return lax.all_to_all(value, axes, 0, 0, tiled=True)

    pieces = run(split_columns_kernel, (3 * square, LANES), sky_maps, copies=rows_count)
    slabs = exchange_pieces(pieces, "rows")
    cuts, slabs = lax.optimization_barrier((cuts, slabs))
    spectra = run(
        lambda *refs: slab_forward_kernel(local_rows, *refs),
        (groups, 6 * local_rows * SUBLANES, LANES),
        *slabs,
        scratch=(pltpu.VMEM((rows_count, 3 * square, LANES), jnp.float32),),
    )
    spectra = exchange(spectra, both)
    legs = run(
        lambda *refs: legs_kernel(config, *refs),
        (groups, 10 * local_rows * SUBLANES, LANES),
        cuts,
        spectra,
        lane_view(filters, outer, local_rows),
        lane_view(wiener, outer, local_rows),
        *tables,
    )
    legs = exchange(legs, both)
    holder = pltpu.VMEM((total_rows, 2, SUBLANES, LANES), jnp.float32)
    current = run(
        lambda *refs: product_kernel(local_rows, *refs),
        (groups, 2 * local_rows * SUBLANES, LANES),
        legs,
        scratch=(holder, holder),
    )
    current = exchange(current, both)
    estimate = run(
        lambda *refs: estimate_kernel(config, *refs),
        (groups, 2 * local_rows * SUBLANES, LANES),
        cuts,
        current,
        lane_view(response, outer, local_rows),
        *tables,
    )
    estimate = exchange(estimate, both)
    maps = run(
        lambda *refs: slab_inverse_kernel(local_rows, *refs),
        (2 * square, LANES),
        estimate,
        scratch=(pltpu.VMEM((rows_count, 2 * square, LANES), jnp.float32),),
        copies=rows_count,
    )
    maps = exchange_pieces(maps, "rows")
    return run(join_columns_kernel, (2, SUBLANES, sky_maps.shape[2]), *maps)


exact_mode = lax.Precision.HIGHEST


def split_factor(length):
    best_first = 1
    for divisor in range(1, math.isqrt(length) + 1):
        if length % divisor == 0:
            best_first = divisor
    return (best_first, length // best_first)


def phase_table(left_index, right_index, period, direction):
    product = left_index[:, None] * right_index[None, :] % period
    angles = direction * 2.0 * math.pi / period * product.astype(jnp.float32)
    return (jnp.cos(angles), jnp.sin(angles))


def complex_einsum(formula, data_pair, table_pair):
    data_real, data_imag = data_pair
    table_real, table_imag = table_pair
    real_out = jnp.einsum(formula, data_real, table_real, precision=exact_mode)
    imag_out = jnp.einsum(formula, data_real, table_imag, precision=exact_mode)
    if data_imag is not None:
        real_out = real_out - jnp.einsum(formula, data_imag, table_imag, precision=exact_mode)
        imag_out = imag_out + jnp.einsum(formula, data_imag, table_real, precision=exact_mode)
    return (real_out, imag_out)


def complex_mul(left_pair, right_pair):
    return (
        left_pair[0] * right_pair[0] - left_pair[1] * right_pair[1],
        left_pair[0] * right_pair[1] + left_pair[1] * right_pair[0],
    )


def conj_mul(left_pair, right_pair):
    return (
        left_pair[0] * right_pair[0] + left_pair[1] * right_pair[1],
        left_pair[0] * right_pair[1] - left_pair[1] * right_pair[0],
    )


def row_transform(data_pair, direction):
    batch_len, length, block_width = data_pair[0].shape
    outer_len, inner_len = split_factor(length)
    outer_ids = jnp.arange(outer_len, dtype=jnp.int32)
    inner_ids = jnp.arange(inner_len, dtype=jnp.int32)
    real_in = data_pair[0].reshape(batch_len, outer_len, inner_len, block_width)
    imag_in = None
    if data_pair[1] is not None:
        imag_in = data_pair[1].reshape(batch_len, outer_len, inner_len, block_width)
    middle = complex_einsum(
        "bjmc,jk->bkmc", (real_in, imag_in), phase_table(outer_ids, outer_ids, outer_len, direction)
    )
    twiddle = phase_table(outer_ids, inner_ids, length, direction)
    middle = complex_mul(middle, (twiddle[0][None, :, :, None], twiddle[1][None, :, :, None]))
    result = complex_einsum(
        "bkmc,mq->bqkc", middle, phase_table(inner_ids, inner_ids, inner_len, direction)
    )
    norm_factor = 1.0 if direction < 0 else 1.0 / length
    return (
        result[0].reshape(batch_len, length, block_width) * norm_factor,
        result[1].reshape(batch_len, length, block_width) * norm_factor,
    )


def block_order(groups, fields_count):
    positions = jnp.arange(groups, dtype=jnp.int32)
    blocks = positions % fields_count * (groups // fields_count) + positions // fields_count
    return (positions, blocks)


def column_forward(data_pair, groups, fields_count):
    batch_len, local_rows, total_len = data_pair[0].shape
    block_width = total_len // groups
    positions, blocks = block_order(groups, fields_count)
    column_ids = jnp.arange(block_width, dtype=jnp.int32)
    shaped = (
        data_pair[0].reshape(batch_len, local_rows, groups, block_width),
        data_pair[1].reshape(batch_len, local_rows, groups, block_width),
    )
    middle = complex_einsum("brpc,pk->brkc", shaped, phase_table(blocks, positions, groups, -1.0))
    twiddle = phase_table(positions, column_ids, total_len, -1.0)
    middle = complex_mul(middle, (twiddle[0][None, None], twiddle[1][None, None]))
    result = complex_einsum(
        "brkc,cq->brqk", middle, phase_table(column_ids, column_ids, block_width, -1.0)
    )
    return (
        result[0].reshape(batch_len, local_rows, total_len),
        result[1].reshape(batch_len, local_rows, total_len),
    )


def column_inverse(data_pair, groups, fields_count):
    batch_len, local_rows, total_len = data_pair[0].shape
    block_width = total_len // groups
    positions, blocks = block_order(groups, fields_count)
    column_ids = jnp.arange(block_width, dtype=jnp.int32)
    shaped = (
        data_pair[0].reshape(batch_len, local_rows, block_width, groups),
        data_pair[1].reshape(batch_len, local_rows, block_width, groups),
    )
    middle = complex_einsum(
        "brqk,qc->brkc", shaped, phase_table(column_ids, column_ids, block_width, 1.0)
    )
    twiddle = phase_table(positions, column_ids, total_len, 1.0)
    middle = complex_mul(middle, (twiddle[0][None, None], twiddle[1][None, None]))
    result = complex_einsum("brkc,kp->brpc", middle, phase_table(positions, blocks, groups, 1.0))
    norm_factor = 1.0 / total_len
    return (
        result[0].reshape(batch_len, local_rows, total_len) * norm_factor,
        result[1].reshape(batch_len, local_rows, total_len) * norm_factor,
    )


def general_body(sky_maps, band_cuts, filters, wiener, response):
    rows_count = lax.axis_size("rows")
    fields_count = lax.axis_size("fields")
    groups = rows_count * fields_count
    local_rows = filters.shape[1]
    total_rows = local_rows * groups
    NC = filters.shape[2]
    row_ratio = NC // total_rows

    def forward_columns(stacked):
        return jnp.stack(column_forward((stacked[0], stacked[1]), groups, fields_count))

    def inverse_slabs(stacked):
        return jnp.stack(row_transform((stacked[0], stacked[1]), 1.0))

    def inverse_columns(stacked):
        return jnp.stack(column_inverse((stacked[0], stacked[1]), groups, fields_count))

    def to_frequency(stacked):
        batch_len = stacked.shape[1]
        block_width = stacked.shape[3]
        shaped = stacked.reshape(
            2, batch_len, rows_count, fields_count, local_rows, 1, 1, block_width
        )
        arrived = lax.all_to_all(
            lax.all_to_all(shaped, "rows", split_axis=2, concat_axis=5, tiled=True),
            "fields",
            split_axis=3,
            concat_axis=6,
            tiled=True,
        )
        result = forward_columns(arrived.reshape(2, batch_len, local_rows, groups * block_width))
        return result

    def to_space(stacked):
        batch_len = stacked.shape[1]
        block_width = stacked.shape[3] // groups
        shaped = stacked.reshape(
            2, batch_len, 1, 1, local_rows, rows_count, fields_count, block_width
        )
        arrived = lax.all_to_all(
            lax.all_to_all(shaped, "rows", split_axis=5, concat_axis=2, tiled=True),
            "fields",
            split_axis=6,
            concat_axis=3,
            tiled=True,
        )
        result = inverse_slabs(arrived.reshape(2, batch_len, total_rows, block_width))
        return result

    slab_spectra = jnp.stack(
        row_transform(
            (lax.all_to_all(sky_maps, "rows", split_axis=2, concat_axis=1, tiled=True), None), -1.0
        )
    )
    sky_spectra = to_frequency(slab_spectra)
    row_ids = lax.axis_index(("rows", "fields")) * local_rows + jnp.arange(
        local_rows, dtype=jnp.int32
    )
    freq_rows = jnp.where(row_ids < total_rows // 2, row_ids, row_ids - total_rows)[:, None]
    column_ids = jnp.arange(NC, dtype=jnp.int32)
    freq_cols = jnp.where(column_ids < NC // 2, column_ids, column_ids - NC)[None, :]
    scaled_rows = row_ratio * freq_rows
    radius_sq = freq_cols * freq_cols + scaled_rows * scaled_rows

    def band_mask(lower_cut, upper_cut):
        inside = (radius_sq >= lower_cut * lower_cut) & (radius_sq <= upper_cut * upper_cut)
        return inside.astype(jnp.float32)

    mask_temp = band_mask(band_cuts[0], band_cuts[1])
    mask_pol = band_mask(band_cuts[2], band_cuts[3])
    mask_out = band_mask(band_cuts[4], band_cuts[5])
    radius_floor = jnp.maximum(radius_sq, 1).astype(jnp.float32)
    cos_two = (freq_cols * freq_cols - scaled_rows * scaled_rows).astype(jnp.float32) / radius_floor
    sin_two = (2 * freq_cols * scaled_rows).astype(jnp.float32) / radius_floor
    along_x = (2 * freq_cols).astype(jnp.float32) / NC
    along_y = (2 * freq_rows).astype(jnp.float32) / total_rows
    raising = (-along_y + 0.0 * along_x, along_x + 0.0 * along_y)
    lowering = (along_y + 0.0 * along_x, along_x + 0.0 * along_y)
    rotation = (cos_two, sin_two)
    temp_modes = (sky_spectra[0, 0], sky_spectra[1, 0])
    stokes_q = (sky_spectra[0, 1], sky_spectra[1, 1])
    stokes_u = (sky_spectra[0, 2], sky_spectra[1, 2])
    e_modes = (
        -(cos_two * stokes_q[0] + sin_two * stokes_u[0]),
        -(cos_two * stokes_q[1] + sin_two * stokes_u[1]),
    )
    b_modes = (
        sin_two * stokes_q[0] - cos_two * stokes_u[0],
        sin_two * stokes_q[1] - cos_two * stokes_u[1],
    )
    temp_weight = mask_temp * filters[0]
    e_weight = mask_pol * filters[1]
    b_weight = mask_pol * filters[2]
    temp_bar = (temp_weight * temp_modes[0], temp_weight * temp_modes[1])
    e_bar = (e_weight * e_modes[0], e_weight * e_modes[1])
    b_bar = (b_weight * b_modes[0], b_weight * b_modes[1])
    grad_temp = complex_mul(raising, (wiener[0] * temp_bar[0], wiener[0] * temp_bar[1]))
    pol_sum = complex_mul((e_bar[0] - b_bar[1], e_bar[1] + b_bar[0]), rotation)
    pol_bar = (-pol_sum[0], -pol_sum[1])
    pol_rot = complex_mul((wiener[1] * e_bar[0], wiener[1] * e_bar[1]), rotation)
    pol_wiener = (-pol_rot[0], -pol_rot[1])
    spin_three = complex_mul(raising, pol_wiener)
    spin_one = complex_mul(lowering, pol_wiener)
    leg_spectra = jnp.stack(
        [
            jnp.stack([temp_bar[0], grad_temp[0], pol_bar[0], spin_three[0], spin_one[0]]),
            jnp.stack([temp_bar[1], grad_temp[1], pol_bar[1], spin_three[1], spin_one[1]]),
        ]
    )
    leg_maps = to_space(inverse_columns(leg_spectra))
    temp_leg = (leg_maps[0, 0], leg_maps[1, 0])
    grad_leg = (leg_maps[0, 1], leg_maps[1, 1])
    pol_leg = (leg_maps[0, 2], leg_maps[1, 2])
    three_leg = (leg_maps[0, 3], leg_maps[1, 3])
    one_leg = (leg_maps[0, 4], leg_maps[1, 4])
    temp_term = complex_mul(temp_leg, grad_leg)
    raise_term = conj_mul(pol_leg, three_leg)
    lower_term = conj_mul(one_leg, pol_leg)
    current = (
        temp_term[0] + 0.5 * (raise_term[0] + lower_term[0]),
        temp_term[1] + 0.5 * (raise_term[1] + lower_term[1]),
    )
    current_rows = jnp.stack(row_transform((current[0][None], current[1][None]), -1.0))
    current_modes = to_frequency(current_rows)
    out_weight = mask_out * response
    estimate_modes = complex_mul(
        lowering, (out_weight * current_modes[0, 0], out_weight * current_modes[1, 0])
    )
    estimate_stack = jnp.stack([estimate_modes[0][None], estimate_modes[1][None]])
    estimate_maps = to_space(inverse_columns(estimate_stack))
    slab_result = estimate_maps[:, 0]
    return lax.all_to_all(slab_result, "rows", split_axis=1, concat_axis=2, tiled=True)


def fits_tiles(sky_maps, band_cuts, filters, wiener, response):
    groups = lax.axis_size("rows") * lax.axis_size("fields")
    return (
        sky_maps.shape[1] == SUBLANES
        and filters.shape[2] // groups == SUBLANES * LANES
        and filters.shape[2] == LANES * LANES
        and lax.axis_size("rows") & (lax.axis_size("rows") - 1) == 0
    )


def body(*operands):
    return tiled_body(*operands) if fits_tiles(*operands) else general_body(*operands)


def solution(mesh):
    placed = (
        P("sims", "rows", "fields"),
        P(),
        P(None, ("rows", "fields"), None),
        P(None, ("rows", "fields"), None),
        P(("rows", "fields"), None),
    )
    return jax.shard_map(
        body, mesh=mesh, in_specs=placed, out_specs=P("sims", "rows", "fields"), check_vma=False
    )
```
